256 devices in a mesh: expert: 8 (over x, core), shard: 32 (over z, y).
Axes of the slice: x: 4, y: 4, z: 8, core: 2. Of those that a mesh axis runs over, the one named last changes fastest.
Arguments:
- train_down: float32 [16, 6400, 4096], P('expert', None, 'shard'), may hold values from -0.15625 to 0.15625
- other_down: bfloat16 [16, 6400, 4096], P('expert', None, 'shard'), may hold values from -0.0390625 to 0.0390625
- router_weight: float32 [4096, 16], P('shard', 'expert'), may hold values from -0.09375 to 0.09375
- router_gain: float32 [4096], P('shard'), may hold values from 0.25 to 1.75
Outputs:
- ready_down: bfloat16 [16, 6400, 4096], P('expert', 'shard')
- scale_down: float32 [16, 6400], P('expert', 'shard')
- serve_router: bfloat16 [4096, 16], replicated
The draws below stay inside these ranges and needn't reach their ends.
All inputs are finite; a program needn't handle non-finite values. Where the reference program divides by a largest or mean magnitude, that divisor is 1e-20 or more.
Results may differ from the reference program's by a relative error of at most 0.001.
Values may be sent and summed in bfloat16 or wider, within the bound.
A program may use at most 64 MiB of HBM per device.

```python
import jax
import jax.numpy as jnp

EXPERTS = 16
D_MODEL = 4096
D_EXPERT = 6400


def spiked(array, rng, source, target, blocks, factor):
    owner, partner = [(jnp.arange(array.shape[axis_at]) // (array.shape[axis_at] // blocks)).reshape([-1 if axis == axis_at else 1 for axis in range(array.ndim)]) for axis_at in (source, target)]
    chosen = jax.random.permutation(rng, blocks)[partner]
    strong = (owner == chosen) | (owner == (partner + blocks // 2) % blocks)
    return jnp.where(strong, factor * array, array)


def block_levels(stream_key, dims, pieces, smallest, high):
    factor_of = 1.0
    for axis_at, parts in pieces:
        draws = jax.random.uniform(jax.random.fold_in(jax.random.fold_in(stream_key, 6), axis_at), (parts,), jnp.float32, smallest / len(pieces), high / len(pieces))
        factor_of = factor_of * jnp.repeat(jnp.exp(draws), dims[axis_at] // parts).reshape((-1,) + (1,) * (len(dims) - 1 - axis_at))
    return factor_of


def noise(key, dims, width, reach, pieces=(), dtype=jnp.bfloat16):
    drawn = width * jax.random.normal(key, dims, jnp.float32)
    if pieces:
        drawn = drawn * block_levels(key, dims, pieces, -0.22, 0.18)
    return jnp.clip(drawn, -reach, reach).astype(dtype)


def noise_with(rng, dims, width, reach, pieces, heavy, dtype=jnp.bfloat16):
    values = width * jax.random.normal(rng, dims, jnp.float32)
    if pieces:
        values = values * block_levels(rng, dims, pieces, -0.22, 0.18)
    return jnp.clip(spiked(values, jax.random.fold_in(rng, 3), *heavy), -reach, reach).astype(dtype)


def setup_inputs(seed: int = 0) -> dict:
    arg_keys = jax.random.split(jax.random.key(seed), 5)
    return {
        "train_down": noise_with(arg_keys[0], (EXPERTS, D_EXPERT, D_MODEL), D_EXPERT ** -0.5, 0.15625, ((0, 8), (2, 32)), (2, 1, 32, 2.75), jnp.float32),
        "other_down": noise(arg_keys[1], (EXPERTS, D_EXPERT, D_MODEL), (D_EXPERT * 4) ** -0.5, 0.0390625, ((0, 8), (2, 32))),
        "router_weight": noise(arg_keys[2], (D_MODEL, EXPERTS), D_MODEL ** -0.5, 0.09375, ((0, 32), (1, 8)), jnp.float32),
        "router_gain": jnp.clip(1.0 + 0.15 * jax.random.normal(arg_keys[3], (D_MODEL,), jnp.float32), 0.25, 1.75),
    }


def reference(train_down, other_down, router_weight, router_gain):
    latest_down = train_down + other_down.astype(jnp.float32)
    scale_down = jnp.max(jnp.abs(latest_down), axis=2)
    ready_down = (latest_down / jnp.expand_dims(scale_down, 2)).astype(jnp.bfloat16)
    serve_router = (router_weight * router_gain[:, None]).astype(jnp.bfloat16)
    return ready_down, scale_down, serve_router
```

```python
import functools

import jax
import jax.numpy as jnp
from jax import lax
from jax.experimental import pallas as pl
from jax.experimental.pallas import tpu as pltpu
from jax.sharding import PartitionSpec as P

MESH = pl.DeviceIdType.MESH
NZ, NY = 8, 4
LANES = 128


def peer_of(me, k):
    h = (k // NY + 1) // 2
    dz = h * (2 * ((k // NY) % 2) - 1)
    return ((me // NY + dz + NZ) % NZ) * NY + (me % NY + k) % NY


def exchange(train, other, weight, gain, out, scale, router,
             latest, late, sendbuf, maxima, seen, whole, scales,
             load_sem, m_send, m_recv, s_send, s_recv, d_send, d_recv, r_send, r_recv, e_send, e_recv):
    me, ex = lax.axis_index("shard"), lax.axis_index("expert")
    shards, experts = lax.axis_size("shard"), lax.axis_size("expert")
    rows = train.shape[1] // shards
    second = rows - LANES
    chunks = load_sem.shape[1]
    chunk = train.shape[1] // chunks

    barrier = pltpu.get_barrier_semaphore()

    def greet(k, c):
        pl.semaphore_signal(barrier, inc=1, device_id={"shard": (me + k) % shards}, device_id_type=MESH)
        return c

    lax.fori_loop(1, shards, greet, 0)

    def greet_expert(k, c):
        pl.semaphore_signal(barrier, inc=1, device_id={"expert": (ex + k) % experts}, device_id_type=MESH)
        return c

    lax.fori_loop(1, experts, greet_expert, 0)

    loads = []
    for c in range(chunks):
        at = pl.ds(c * chunk, chunk)
        a = pltpu.make_async_copy(train.at[:, at], latest.at[:, at], load_sem.at[0, c])
        b = pltpu.make_async_copy(other.at[:, at], late.at[:, at], load_sem.at[1, c])
        a.start()
        b.start()
        loads.append((a, b))

    part = (weight[...] * gain[...]).astype(jnp.bfloat16)
    mine = pl.ds(pl.multiple_of(me * LANES, LANES), LANES)
    router[ex, :, mine] = part

    def block_max(d, j):
        start = pl.multiple_of(d * rows + (second if j % 2 else 0), 8)
        x = jnp.abs(latest[j // 2, pl.ds(start, LANES), :])
        return jnp.max(x.T, axis=0, keepdims=True)

    for c in range(chunks):
        for load in loads[c]:
            load.wait()
        step = 160

        def add(i, carry):
            at = pl.ds(pl.multiple_of(c * chunk + i * step, 32), step)
            for e in range(2):
                latest[e, at, :] = latest[e, at, :] + late[e, at, :].astype(jnp.float32)
            return carry

        lax.fori_loop(0, chunk // step, add, 0)

        def one(d, carry):
            for j in range(4):
                maxima[d, j:j + 1, :] = block_max(d, j)
            return carry

        lax.fori_loop(c * chunk // rows, (c + 1) * chunk // rows, one, 0)

    pl.semaphore_wait(barrier, shards + experts - 2)

    def max_copy(d):
        return pltpu.make_async_remote_copy(
            maxima.at[d], seen.at[me], m_send.at[d], m_recv.at[me], device_id={"shard": d}, device_id_type=MESH)

    def max_from(s):
        return pltpu.make_async_remote_copy(
            maxima.at[s], seen.at[s], m_send.at[s], m_recv.at[s], device_id={"shard": s}, device_id_type=MESH)

    def send_max(k, c):
        max_copy(peer_of(me, shards - k)).start()
        return c

    lax.fori_loop(1, shards, send_max, 0)
    seen[me] = maxima[me]

    def router_copy(d):
        return pltpu.make_async_remote_copy(
            router.at[ex, :, mine], router.at[ex, :, mine], r_send.at[d], r_recv.at[me],
            device_id={"shard": d}, device_id_type=MESH)

    def router_from(s):
        at = pl.ds(pl.multiple_of(s * LANES, LANES), LANES)
        return pltpu.make_async_remote_copy(
            router.at[ex, :, at], router.at[ex, :, at], r_send.at[s], r_recv.at[s],
            device_id={"shard": s}, device_id_type=MESH)

    def wait_max(k, c):
        max_from(peer_of(me, k)).wait_recv()
        return c

    lax.fori_loop(1, shards, wait_max, 0)
    whole[...] = jnp.max(seen[...], axis=0)

    def scale_copy(d):
        return pltpu.make_async_remote_copy(
            whole, scales.at[me], s_send.at[d], s_recv.at[me], device_id={"shard": d}, device_id_type=MESH)

    def scale_from(s):
        return pltpu.make_async_remote_copy(
            whole, scales.at[s], s_send.at[s], s_recv.at[s], device_id={"shard": s}, device_id_type=MESH)

    def send_scale(k, c):
        scale_copy(peer_of(me, k)).start()
        return c

    lax.fori_loop(1, shards, send_scale, 0)
    scales[me] = whole[...]
    for e in range(2):
        scale[e:e + 1, 0:LANES] = whole[2 * e:2 * e + 1, :]
        scale[e:e + 1, LANES:rows] = whole[2 * e + 1:2 * e + 2, LANES - second:LANES]

    def send_router(k, c):
        router_copy(peer_of(me, k)).start()
        return c

    lax.fori_loop(1, shards, send_router, 0)

    def ready(d, j):
        column = jnp.broadcast_to(1.0 / scales[d, j:j + 1, :], (LANES, LANES)).T
        if j % 2:
            start, column = d * rows + LANES, column[LANES - second:]
        else:
            start = d * rows
        return latest[j // 2, pl.ds(pl.multiple_of(start, 8), column.shape[0]), :] * column

    def data_copy(d):
        return pltpu.make_async_remote_copy(
            sendbuf.at[d], out.at[:, :, mine], d_send.at[d], d_recv.at[me], device_id={"shard": d}, device_id_type=MESH)

    def data_from(s):
        at = pl.ds(pl.multiple_of(s * LANES, LANES), LANES)
        return pltpu.make_async_remote_copy(
            sendbuf.at[s], out.at[:, :, at], d_send.at[s], d_recv.at[s], device_id={"shard": s}, device_id_type=MESH)

    def prepare(d):
        for j in range(4):
            x = ready(d, j).astype(jnp.bfloat16)
            first = LANES if j % 2 else 0
            sendbuf[d, j // 2, first:first + x.shape[0], :] = x

    def send_data(k, c):
        d = peer_of(me, k)
        scale_from(d).wait_recv()
        prepare(d)

        @pl.when(k > 1)
        def _():
            data_copy(peer_of(me, k - 1)).start()

        return c

    lax.fori_loop(1, shards, send_data, 0)
    for j in range(4):
        x = ready(me, j).astype(jnp.bfloat16)
        first = LANES if j % 2 else 0
        out[j // 2, first:first + x.shape[0], mine] = x
    data_copy(peer_of(me, shards - 1)).start()

    def wait_router(k, c):
        router_from(peer_of(me, k)).wait_recv()
        return c

    lax.fori_loop(1, shards, wait_router, 0)

    def expert_copy(e):
        return pltpu.make_async_remote_copy(
            router.at[ex], router.at[ex], e_send.at[e], e_recv.at[ex], device_id={"expert": e}, device_id_type=MESH)

    def expert_from(e):
        return pltpu.make_async_remote_copy(
            router.at[e], router.at[e], e_send.at[e], e_recv.at[e], device_id={"expert": e}, device_id_type=MESH)

    def send_expert(k, c):
        expert_copy((ex + k) % experts).start()
        return c

    lax.fori_loop(1, experts, send_expert, 0)

    def finish_early(k, c):
        d = peer_of(me, k)
        max_copy(d).wait_send()
        scale_copy(d).wait_send()
        router_copy(d).wait_send()
        return c

    lax.fori_loop(1, shards, finish_early, 0)

    def finish_expert(k, c):
        e = (ex + k) % experts
        expert_copy(e).wait_send()
        expert_from(e).wait_recv()
        return c

    lax.fori_loop(1, experts, finish_expert, 0)

    def finish(k, c):
        d = peer_of(me, k)
        data_copy(d).wait_send()
        data_from(d).wait_recv()
        return c

    lax.fori_loop(1, shards, finish, 0)


def store(out_in, scale_in, router_in, out, scale, router, columns, sem):
    rows = out.shape[1]
    copies = [pltpu.make_async_copy(out_in.at[e], out.at[e], sem.at[e]) for e in range(2)]
    for copy in copies:
        copy.start()
    keep = pltpu.make_async_copy(scale_in, scale, sem.at[2])
    keep.start()
    for e in range(router_in.shape[0]):
        columns[2 * e:2 * e + 2, :] = router_in[e]
    last = pltpu.make_async_copy(columns, router, sem.at[3])
    last.start()
    for copy in (*copies, keep, last):
        copy.wait()


def per_device(train_down, other_down, router_weight, router_gain):
    shards, experts = lax.axis_size("shard"), lax.axis_size("expert")
    each, length, width = train_down.shape
    rows = length // shards
    vmem = pl.BlockSpec(memory_space=pltpu.VMEM)
    hbm = pl.BlockSpec(memory_space=pl.ANY)
    bf16, f32 = jnp.bfloat16, jnp.float32
    dma = pltpu.SemaphoreType.DMA
    blocks = (4, LANES)
    out, scale, router = pl.pallas_call(
        exchange,
        out_shape=(
            jax.ShapeDtypeStruct((each, rows, width * shards), bf16),
            jax.ShapeDtypeStruct((each, rows), f32),
            jax.ShapeDtypeStruct((experts, each, shards * LANES), bf16),
        ),
        in_specs=[hbm, hbm, vmem, vmem],
        out_specs=(vmem, vmem, vmem),
        scratch_shapes=[
            pltpu.VMEM((each, length, width), f32),
            pltpu.VMEM((each, length, width), bf16),
            pltpu.VMEM((shards, each, rows, width), bf16),
            pltpu.VMEM((shards, *blocks), f32),
            pltpu.VMEM((shards, *blocks), f32),
            pltpu.VMEM(blocks, f32),
            pltpu.VMEM((shards, *blocks), f32),
            dma((2, 8)),
            *[dma((shards,)) for _ in range(8)],
            dma((experts,)),
            dma((experts,)),
        ],
        compiler_params=pltpu.CompilerParams(
            collective_id=0, has_side_effects=True, vmem_limit_bytes=48 * 1024 * 1024
        ),
        name="exchange",
    )(train_down, other_down, router_weight.T, router_gain.reshape(1, LANES))
    out, scale, router = pl.pallas_call(
        store,
        out_shape=(
            jax.ShapeDtypeStruct(out.shape, bf16),
            jax.ShapeDtypeStruct(scale.shape, f32),
            jax.ShapeDtypeStruct((experts * each, shards * LANES), bf16),
        ),
        in_specs=[vmem] * 3,
        out_specs=[hbm] * 3,
        scratch_shapes=[pltpu.VMEM((experts * each, shards * LANES), bf16), dma((4,))],
        compiler_params=pltpu.CompilerParams(vmem_limit_bytes=8 * 1024 * 1024),
        name="store",
    )(out, scale, router)
    return out, scale, router.T


def solution(mesh):
    in_specs = (
        P("expert", None, "shard"),
        P("expert", None, "shard"),
        P("shard", "expert"),
        P("shard"),
    )
    out_specs = (P("expert", "shard", None), P("expert", "shard"), P())
    return jax.shard_map(
        per_device, mesh=mesh, in_specs=in_specs, out_specs=out_specs, check_vma=False
    )
```
